32 devices in a mesh: blk: 8 (over z, x), rows: 4 (over y, core).
Axes of the slice: x: 2, y: 2, z: 4, core: 2. Of those that a mesh axis runs over, the one named last changes fastest.
Arguments:
- centers: int32 [512, 1], P(('blk', 'rows')), may hold values from 0 to 127, as said below
- gates_used: int32 [512], P(('blk', 'rows')), may hold values from 12 to 40
- jacobian: bfloat16 [512, 3, 40, 256], P(('blk', 'rows')), may hold values from -0.3984375 to 0.3984375
- weights: bfloat16 [512, 40], P(('blk', 'rows')), may hold values from 0.099609375 to 1
Outputs:
- hessian_band: float32 [128, 3, 256, 256], P(('blk', 'rows'))
The draws below stay inside these ranges and needn't reach their ends.
Inputs may be any that keep to these rules, and one draw needn't show every extreme that they name: `centers`: cell block c is owned by blk index c // 16. Among the soundings of one device at most 4 are centred on blocks of one owner, and some owner gets exactly 4 of them; the number a device sends to the owner k places further along blk (cyclically) is the same for all devices of one rows index. Among the soundings of all devices of one rows index at most 2 share a centre block, and some block has exactly 2.
All inputs are finite; a program needn't handle non-finite values.
Results may differ from the reference program's by a relative error of at most 0.0024.
Values may be sent and summed in bfloat16 or wider, within the bound.
No kernel may reach another device: no remote copies, remote signals or barrier semaphores. Data moves between devices by JAX's collectives and lax.ppermute only.
A program may use at most 128 MiB of HBM per device.

```python
import math
import jax
import jax.numpy as jnp
from jax import lax

B = 256
G = 40
FOOT = 3
S_DEV = 16
KB = 16
CAP = 4
CAPB = 2
SOUND = 512
NCB = 128
N_BLK = 8
N_ROWS = 4


def pick_values(key, groups, capacity, take, forced_first, forced_second, forcing):
    first_key, second_key, third_key = jax.random.split(key, 3)
    total = groups * capacity
    slots = jnp.arange(total, dtype=jnp.int32)
    values = slots // capacity
    full_value = jax.random.randint(first_key, (), 0, groups, dtype=jnp.int32)
    scores = jax.random.permutation(second_key, total).astype(jnp.int32) + jnp.where(values == full_value, -total, 0).astype(jnp.int32)
    if forcing:
        forced_slot = (slots == forced_first * capacity) | (slots == forced_second * capacity + (capacity - 1))
        scores = scores + jnp.where(forced_slot, -3 * total, 0).astype(jnp.int32)
    order = jnp.argsort(scores, stable=True)
    chosen = values[order[:take]]
    return chosen[jax.random.permutation(third_key, take)]


def one_rows_index(row_key):
    value_key, place_key, local_key = jax.random.split(row_key, 3)
    distance = pick_values(value_key, N_BLK, CAP, S_DEV, 1, N_BLK // 2, True)
    placing = jax.vmap(lambda one_key: jax.random.permutation(one_key, S_DEV).astype(jnp.int32))(jax.random.split(place_key, N_BLK))
    local_pick = jax.vmap(lambda one_key: pick_values(one_key, KB, CAPB, S_DEV, 0, 0, False))(jax.random.split(local_key, N_BLK))
    owner = (jnp.arange(N_BLK, dtype=jnp.int32)[:, None] + distance[placing]) % N_BLK
    within = local_pick[owner, placing]
    return owner * KB + within


def draw_centers(key, part):
    row_keys = jax.random.split(jax.random.fold_in(key, 31), N_ROWS)
    grid = jax.vmap(one_rows_index)(row_keys)
    return jnp.transpose(grid, (1, 0, 2)).reshape(SOUND, 1).astype(jnp.int32)


def with_ends(drawn, own_key, smallest, top_value):
    longest = drawn.shape.index(max(drawn.shape))
    spots = []
    for shift in (0, 1):
        where = [jax.random.randint(jax.random.fold_in(own_key, axis), (), 0, length) for axis, length in enumerate(drawn.shape)]
        where[longest] = (where[longest] + shift) % drawn.shape[longest]
        spots.append(tuple(where))
    return drawn.at[spots[0]].set(smallest).at[spots[1]].set(top_value)


def shard_levels(own_key, extent, cuts, smallest, largest):
    factor_of = 1.0
    for dim, parts in cuts:
        steps = jax.random.uniform(jax.random.fold_in(jax.random.fold_in(own_key, 6), dim), (parts,), jnp.float32, smallest / len(cuts), largest / len(cuts))
        factor_of = factor_of * jnp.repeat(jnp.exp(steps), extent[dim] // parts).reshape((-1,) + (1,) * (len(extent) - 1 - dim))
    return factor_of


def bell_draw(key, shape, scale, limit, shards=(), kind=jnp.bfloat16):
    loudness = shard_levels(key, shape, shards, -0.22, 0.18) if shards else 1.0
    result = jax.random.normal(key, shape, jnp.float32) * scale * loudness
    return jnp.minimum(jnp.maximum(result, -limit), limit).astype(kind)


def setup_inputs(seed: int = 0) -> dict:
    seeds = jax.random.split(jax.random.key(seed), 5)
    return {
        "centers": draw_centers(jax.random.fold_in(seeds[4], 71), 0),
        "gates_used": with_ends(jax.random.randint(seeds[1], (SOUND,), 12, G + 1), jax.random.fold_in(seeds[1], 1), 12, G).astype(jnp.int32),
        "jacobian": bell_draw(seeds[2], (SOUND, FOOT, G, B), 0.06, 0.3984375, ((0, 32),)),
        "weights": jnp.clip(jnp.exp(math.log(1.0) - 2.306499 * jax.random.uniform(seeds[3], (SOUND, G), jnp.float32) ** shard_levels(seeds[3], (SOUND, G), ((0, 32),), -0.2, 0.2)), 0.099609375, 1.0).astype(jnp.bfloat16),
    }


def reference(centers, gates_used, jacobian, weights):
    centre_ids = centers[:, 0].astype(jnp.int32)
    gate_live = jnp.arange(G, dtype=jnp.int32)[None, :] < gates_used.astype(jnp.int32)[:, None]
    weight_live = jnp.where(gate_live, weights.astype(jnp.float32), jnp.zeros((), jnp.float32))
    window = CAPB * N_ROWS
    sort_order = jnp.argsort(centre_ids, stable=True).astype(jnp.int32)
    order_pad = jnp.concatenate([sort_order, jnp.zeros((window,), jnp.int32)])
    centre_pad = jnp.concatenate([centre_ids[sort_order], jnp.full((window,), NCB + 7, jnp.int32)])
    footprint = jnp.arange(FOOT, dtype=jnp.int32)

    def one_row(row_id):
        blocks = [jnp.zeros((B, B), jnp.float32) for offset in range(FOOT)]
        for lead_pos in range(FOOT):
            centre = (row_id - lead_pos + 1).astype(jnp.int32)
            window_start = jnp.sum((centre_ids < centre).astype(jnp.int32)).astype(jnp.int32)
            picked = lax.dynamic_slice(order_pad, (window_start,), (window,))
            in_window = (lax.dynamic_slice(centre_pad, (window_start,), (window,)) == centre).astype(jnp.float32)
            grid_pos = centre + footprint - 1
            inside = ((grid_pos >= 0) & (grid_pos < NCB)).astype(jnp.float32)
            rows_jac = jacobian[picked].astype(jnp.float32) * in_window[:, None, None, None] * inside[None, :, None, None]
            masked = rows_jac.astype(jnp.bfloat16)
            scaled = (rows_jac * weight_live[picked][:, None, :, None]).astype(jnp.bfloat16)
            for offset in range(FOOT - lead_pos):
                blocks[offset] = blocks[offset] + jnp.dot(scaled[:, lead_pos].reshape(-1, B).T, masked[:, lead_pos + offset].reshape(-1, B), preferred_element_type=jnp.float32)
        return jnp.stack(blocks)

    return lax.map(one_row, jnp.arange(NCB, dtype=jnp.int32))
```

```python
import functools

import jax
import jax.numpy as jnp
from jax import lax
from jax.experimental import pallas as pl
from jax.experimental.pallas import tpu as pltpu
from jax.sharding import PartitionSpec as P

KB = 16
ID_LANE = 64
META = 8


ANY = pl.BlockSpec(memory_space=pl.ANY)
SMEM = pl.BlockSpec(memory_space=pltpu.SMEM)
VMEM = pl.BlockSpec(memory_space=pltpu.VMEM)


def lanes(shape):
    return lax.broadcasted_iota(jnp.int32, shape, len(shape) - 1)


def pack_kernel(cfg, start, gates, meta, centers, *refs):
    count, cap, foot, relative = cfg
    if meta:
        used, weights, jac, out, seen, rows, staged, wide, sems, meta_sem = refs
        weight_rows, gate_len = weights.shape
        wide[...] = jnp.zeros_like(wide)
        wide[:, :gate_len] = weights[...].astype(jnp.float32)
        rows[...] = jnp.zeros_like(rows)
    else:
        jac, out, seen, sems = refs
    mine = lax.axis_index("blk")
    sounds = jac.shape[0]
    for place in range(count):
        seen[place] = 0
    copies = []
    for s in range(sounds):
        centre = centers[s]
        owner = centre // KB
        place = owner
        if relative:
            place = owner - mine
            place = jnp.where(place < 0, place + count, place)
        rank = seen[place]
        seen[place] = rank + 1
        for i in range(foot):
            top = pl.multiple_of((rank * foot + i) * gates, 8)
            copy = pltpu.make_async_copy(
                jac.at[s, i, pl.ds(start, gates), :],
                out.at[place, pl.ds(top, gates), :],
                sems.at[s * foot + i],
            )
            copy.start()
            copies.append(copy)
        if meta:
            at = lanes((1, 128))
            row = jnp.where(at < used[s], wide[pl.ds(s, 1), :], 0.0)
            mark = ID_LANE + (place if relative else mine)
            within = (centre - owner * KB + 1).astype(jnp.float32)
            row = jnp.where(at == mark, within, row)
            rows[pl.ds(place * META + rank, 1), :] = row
    if meta:
        width = staged.shape[2]
        staged[:, :, :128] = rows[...].astype(jnp.bfloat16).reshape(count, META, 128)
        staged[:, :, 128:] = jnp.zeros((count, META, width - 128), jnp.bfloat16)
        copy = pltpu.make_async_copy(
            staged, out.at[:, pl.ds(cap * foot * gates, META), :], meta_sem
        )
        copy.start()
        copies.append(copy)
    for copy in copies:
        copy.wait()


def pack(cfg, start, gates, meta, centers, used, weights, jac):
    count, cap, foot, relative = cfg
    sounds, _, _, cells = jac.shape
    tall = cap * foot * gates + (META if meta else 0)
    scratch = [pltpu.SMEM((count,), jnp.int32)]
    if meta:
        scratch += [
            pltpu.VMEM((count * META, 128), jnp.float32),
            pltpu.VMEM((count, META, cells), jnp.bfloat16),
            pltpu.VMEM((sounds, 128), jnp.float32),
        ]
    scratch.append(pltpu.SemaphoreType.DMA((sounds * foot,)))
    if meta:
        scratch.append(pltpu.SemaphoreType.DMA(()))
    args = (centers, used, weights, jac) if meta else (centers, jac)
    return pl.pallas_call(
        functools.partial(pack_kernel, cfg, start, gates, meta),
        out_shape=jax.ShapeDtypeStruct((count, tall, cells), jnp.bfloat16),
        in_specs=[SMEM, SMEM, VMEM, ANY] if meta else [SMEM, ANY],
        out_specs=ANY,
        scratch_shapes=scratch,
        name="pack1" if meta else "pack2",
    )(*args)


def each(count, fn):
    if count <= 32:
        for n in range(count):
            fn(n)
    else:

        def step(n, carry):
            fn(n)
            return carry

        lax.fori_loop(0, count, step, 0)


def first_kernel(cfg, share, bcap, gates, recv, blank, out, table, marks, near, vids, sids, seen, rows, staged, sems, aux):
    count, cap, foot, _ = cfg
    del blank
    span = foot * gates
    slots = share * bcap
    pull = pltpu.make_async_copy(recv.at[:, pl.ds(cap * span, META), :], marks, aux.at[0])
    pull.start()
    for n in range(KB):
        seen[n] = 0
    rows[...] = jnp.zeros_like(rows)
    pull.wait()
    total = jnp.zeros((META, 128), jnp.float32)
    for p in range(count):
        part = marks[p, :, :128].astype(jnp.float32)
        near[pl.ds(p * META, META), :] = part
        total = total + part
    vids[...] = total.astype(jnp.int32)
    ids = pltpu.make_async_copy(vids, sids, aux.at[0])
    ids.start()
    ids.wait()

    def copy_of(n, row, slot):
        p = n // cap
        j = n - p * cap
        return pltpu.make_async_copy(
            recv.at[p, pl.ds(pl.multiple_of(j * span, 8), span), :],
            out.at[row, pl.ds(pl.multiple_of(slot * span, 8), span), :],
            sems.at[n],
        )

    def place(n):
        p = n // cap
        j = n - p * cap
        mark = sids[j, ID_LANE + p]
        table[n] = -1

        @pl.when(mark > 0)
        def _():
            within = mark - 1
            row = within // share
            rank = seen[within]
            seen[within] = rank + 1
            slot = (within - row * share) * bcap + rank
            table[n] = row * slots + slot
            copy_of(n, row, slot).start()
            rows[pl.ds(row * META + slot, 1), :] = near[pl.ds(p * META + j, 1), :]

    each(count * cap, place)
    owners = staged.shape[0]
    staged[:, :, :128] = rows[...].astype(jnp.bfloat16).reshape(owners, META, 128)
    staged[:, :, 128:] = jnp.zeros((owners, META, staged.shape[2] - 128), jnp.bfloat16)
    push = pltpu.make_async_copy(staged, out.at[:, pl.ds(slots * span, META), :], aux.at[1])
    push.start()

    def finish(n):
        @pl.when(table[n] >= 0)
        def _():
            copy_of(n, 0, 0).wait()

    each(count * cap, finish)
    push.wait()


def second_kernel(cfg, slots, gates, table, recv, blank, out, sems):
    count, cap, foot, _ = cfg
    del blank
    span = foot * gates

    def copy_of(n, row, slot):
        p = n // cap
        j = n - p * cap
        return pltpu.make_async_copy(
            recv.at[p, pl.ds(pl.multiple_of(j * span, 8), span), :],
            out.at[row, pl.ds(pl.multiple_of(slot * span, 8), span), :],
            sems.at[n],
        )

    def place(n):
        to = table[n]

        @pl.when(to >= 0)
        def _():
            row = to // slots
            copy_of(n, row, to - row * slots).start()

    def finish(n):
        @pl.when(table[n] >= 0)
        def _():
            copy_of(n, 0, 0).wait()

    each(count * cap, place)
    each(count * cap, finish)


def bucket_first(cfg, owners, share, bcap, gates, recv):
    count, cap, foot, _ = cfg
    cells = recv.shape[2]
    tall = share * bcap * foot * gates + META
    blank = jnp.zeros((owners, tall, cells), jnp.bfloat16)
    return pl.pallas_call(
        functools.partial(first_kernel, cfg, share, bcap, gates),
        out_shape=(
            jax.ShapeDtypeStruct(blank.shape, blank.dtype),
            jax.ShapeDtypeStruct((count * cap,), jnp.int32),
        ),
        in_specs=[ANY, ANY],
        out_specs=(ANY, SMEM),
        scratch_shapes=[
            pltpu.VMEM((count, META, cells), jnp.bfloat16),
            pltpu.VMEM((count * META, 128), jnp.float32),
            pltpu.VMEM((META, 128), jnp.int32),
            pltpu.SMEM((META, 128), jnp.int32),
            pltpu.SMEM((KB,), jnp.int32),
            pltpu.VMEM((owners * META, 128), jnp.float32),
            pltpu.VMEM((owners, META, cells), jnp.bfloat16),
            pltpu.SemaphoreType.DMA((count * cap,)),
            pltpu.SemaphoreType.DMA((2,)),
        ],
        input_output_aliases={1: 0},
        name="mid1",
    )(recv, blank)


def bucket_second(cfg, owners, slots, gates, table, recv):
    count, cap, foot, _ = cfg
    cells = recv.shape[2]
    blank = jnp.zeros((owners, slots * foot * gates, cells), jnp.bfloat16)
    return pl.pallas_call(
        functools.partial(second_kernel, cfg, slots, gates),
        out_shape=jax.ShapeDtypeStruct(blank.shape, blank.dtype),
        in_specs=[SMEM, ANY, ANY],
        out_specs=ANY,
        scratch_shapes=[pltpu.SemaphoreType.DMA((count * cap,))],
        input_output_aliases={2: 0},
        name="mid2",
    )(table, recv, blank)


def weight_columns(first, slots, span):
    cols = []
    for q in range(first.shape[0]):
        tile = first[q, pl.ds(slots * span, META), :128].astype(jnp.float32)
        cols.append(tile.T)
    return cols


def operands(cols, chunks, block, bcap, foot, i):
    plain, scaled = [], []
    start = 0
    for ref, gates in chunks:
        for q in range(ref.shape[0]):
            for t in range(bcap):
                slot = block * bcap + t
                rows = ref[q, pl.ds((slot * foot + i) * gates, gates), :].astype(jnp.float32)
                plain.append(rows)
                scaled.append(rows * cols[q][start : start + gates, slot : slot + 1])
        start += gates
    return (
        jnp.concatenate(plain, axis=0).astype(jnp.bfloat16),
        jnp.concatenate(scaled, axis=0).astype(jnp.bfloat16),
    )


def cross(left, right):
    return lax.dot_general(
        left, right, (((0,), (0,)), ((), ())), preferred_element_type=jnp.float32
    )


def edge_kernel(cfg, gates, first, second, low, high):
    share, bcap, foot = cfg
    slots = share * bcap
    cols = weight_columns(first, slots, foot * gates[0])
    chunks = ((first, gates[0]), (second, gates[1]))
    found = [operands(cols, chunks, 0, bcap, foot, i) for i in range(foot)]
    for d in range(foot):
        low[d] = cross(found[0][1], found[d][0]).astype(low.dtype)
    last = operands(cols, chunks, share - 1, bcap, foot, foot - 1)
    high[0] = cross(last[1], last[0]).astype(high.dtype)


def main_kernel(cfg, gates, first, second, out, edge, hold, sems):
    share, bcap, foot = cfg
    slots = share * bcap
    total = lax.axis_size("blk") * lax.axis_size("rows")
    me = lax.axis_index("blk") * lax.axis_size("rows") + lax.axis_index("rows")
    keep = (me != total - 1).astype(jnp.float32).astype(jnp.bfloat16)
    cols = weight_columns(first, slots, foot * gates[0])
    chunks = ((first, gates[0]), (second, gates[1]))
    found = {}

    def get(j, i):
        if (j, i) not in found:
            found[j, i] = operands(cols, chunks, j, bcap, foot, i)
        return found[j, i]

    def right(j, i, lead):
        rows = get(j, i)[0]
        if j == share - 1 and i == foot - 1 and lead != i:
            rows = rows * keep
        return rows

    copies = []
    for j in range(share):
        for d in range(foot):
            lefts, rights = [], []
            for lead in range(foot - d):
                source = j - lead + 1
                if 0 <= source < share:
                    lefts.append(get(source, lead)[1])
                    rights.append(right(source, lead + d, lead))
            if j == share - 1 or (j == 0 and d == 0):
                spot = edge.at[0 if j == 0 else 1 + d]
            else:
                spot = hold.at[j * foot + d]
            if lefts:
                spot[...] = cross(jnp.concatenate(lefts, 0), jnp.concatenate(rights, 0))
            else:
                spot[...] = jnp.zeros(spot.shape, jnp.float32)
            if not (j == share - 1 or (j == 0 and d == 0)):
                copy = pltpu.make_async_copy(spot, out.at[j, d], sems.at[j * foot + d])
                copy.start()
                copies.append(copy)
    for copy in copies:
        copy.wait()


def join_kernel(share, foot, edge, from_low, from_high, prior, out, hold, sems):
    del prior
    hold[0] = edge[0] + from_low[0].astype(jnp.float32)
    copies = [pltpu.make_async_copy(hold.at[0], out.at[0, 0], sems.at[0])]
    copies[0].start()
    for d in range(foot):
        hold[1 + d] = edge[1 + d] + from_high[d].astype(jnp.float32)
        copy = pltpu.make_async_copy(hold.at[1 + d], out.at[share - 1, d], sems.at[1 + d])
        copy.start()
        copies.append(copy)
    for copy in copies:
        copy.wait()


def over_blk(packed, relative):
    if not relative:
        return lax.all_to_all(packed, "blk", split_axis=0, concat_axis=0, tiled=True)
    count = packed.shape[0]
    order = sorted(range(1, count), key=lambda k: abs(2 * k - count))
    parts = {0: packed[0:1]}
    for k in order:
        ring = [(n, (n + k) % count) for n in range(count)]
        parts[k] = lax.ppermute(packed[k : k + 1], "blk", ring)
    return jnp.concatenate([parts[k] for k in range(count)], axis=0)


def over_rows(buckets):
    return lax.all_to_all(buckets, "rows", split_axis=0, concat_axis=0, tiled=True)


def on_device(centers, gates_used, jacobian, weights):
    count = lax.axis_size("blk")
    owners = lax.axis_size("rows")
    sounds, foot, gate_len, cells = jacobian.shape
    cap = max(2, 2 * sounds // count)
    bcap = max(2, 2 * sounds // KB)
    share = KB // owners
    slots = share * bcap
    relative = count <= 8
    cfg = (count, cap, foot, relative)
    one = -(-(3 * gate_len // 5) // 8) * 8
    gates = (one, gate_len - one)
    centre_ids = centers[:, 0]

    packed1 = pack(cfg, 0, gates[0], True, centre_ids, gates_used, weights, jacobian)
    packed2 = pack(cfg, gates[0], gates[1], False, centre_ids, gates_used, weights, jacobian)
    arrived1 = over_blk(packed1, relative)
    arrived2 = over_blk(packed2, relative)
    buckets1, table = bucket_first(cfg, owners, share, bcap, gates[0], arrived1)
    first = over_rows(buckets1)
    buckets2 = bucket_second(cfg, owners, slots, gates[1], table, arrived2)
    second = over_rows(buckets2)

    shape = (share, bcap, foot)
    low, high = pl.pallas_call(
        functools.partial(edge_kernel, shape, gates),
        out_shape=(
            jax.ShapeDtypeStruct((foot, cells, cells), jnp.bfloat16),
            jax.ShapeDtypeStruct((1, cells, cells), jnp.bfloat16),
        ),
        in_specs=[VMEM, VMEM],
        out_specs=(VMEM, VMEM),
        name="edge",
    )(first, second)
    total = count * owners
    axes = ("blk", "rows")
    from_high = lax.ppermute(low, axes, [(n, n - 1) for n in range(1, total)])
    from_low = lax.ppermute(high, axes, [(n, n + 1) for n in range(total - 1)])
    out_shape = jax.ShapeDtypeStruct((share, foot, cells, cells), jnp.float32)
    inner, edge = pl.pallas_call(
        functools.partial(main_kernel, shape, gates),
        out_shape=(out_shape, jax.ShapeDtypeStruct((1 + foot, cells, cells), jnp.float32)),
        in_specs=[VMEM, VMEM],
        out_specs=(ANY, VMEM),
        scratch_shapes=[
            pltpu.VMEM((share * foot, cells, cells), jnp.float32),
            pltpu.SemaphoreType.DMA((share * foot,)),
        ],
        name="inner",
    )(first, second)
    return pl.pallas_call(
        functools.partial(join_kernel, share, foot),
        out_shape=out_shape,
        in_specs=[VMEM, VMEM, VMEM, ANY],
        out_specs=ANY,
        scratch_shapes=[
            pltpu.VMEM((1 + foot, cells, cells), jnp.float32),
            pltpu.SemaphoreType.DMA((1 + foot,)),
        ],
        input_output_aliases={3: 0},
        name="join",
    )(edge, from_low, from_high, inner)


def solution(mesh):
    placed = (
        P(("blk", "rows"), None),
        P(("blk", "rows")),
        P(("blk", "rows"), None, None, None),
        P(("blk", "rows"), None),
    )
    return jax.shard_map(
        on_device,
        mesh=mesh,
        in_specs=placed,
        out_specs=P(("blk", "rows"), None, None, None),
        check_vma=False,
    )
```

```python
import functools

import jax
import jax.numpy as jnp
from jax import lax
from jax.experimental import pallas as pl
from jax.experimental.pallas import tpu as pltpu
from jax.sharding import PartitionSpec as P

KB = 16
ID_LANE = 64
META = 8


ANY = pl.BlockSpec(memory_space=pl.ANY)
SMEM = pl.BlockSpec(memory_space=pltpu.SMEM)
VMEM = pl.BlockSpec(memory_space=pltpu.VMEM)


def grant(mib):
    return pltpu.CompilerParams(vmem_limit_bytes=mib << 20)


def lanes(shape):
    return lax.broadcasted_iota(jnp.int32, shape, len(shape) - 1)


def pack_kernel(cfg, start, gates, meta, centers, *refs):
    count, cap, foot, relative = cfg
    if meta:
        used, weights, jac, out, seen, wide = refs
        gate_len = weights.shape[1]
        wide[...] = jnp.zeros_like(wide)
        wide[:, :gate_len] = weights[...].astype(jnp.float32)
        rows = [jnp.zeros((META, 128), jnp.float32)] * count
    else:
        jac, out, seen = refs
    mine = lax.axis_index("blk")
    for place in range(count):
        seen[place] = 0
    if meta:
        held = cap * foot * gates
        out[:, held:, :] = jnp.zeros((count, META, out.shape[2]), out.dtype)
    for s in range(jac.shape[0]):
        centre = centers[s]
        owner = centre // KB
        place = owner
        if relative:
            place = owner - mine
            place = jnp.where(place < 0, place + count, place)
        rank = seen[place]
        seen[place] = rank + 1
        for i in range(foot):
            top = pl.multiple_of((rank * foot + i) * gates, 8)
            out[place, pl.ds(top, gates), :] = jac[s, i, start : start + gates, :]
        if meta:
            at = lanes((META, 128))
            row = jnp.broadcast_to(wide[s : s + 1, :], (META, 128))
            row = jnp.where(at < used[s], row, 0.0)
            mark = ID_LANE + (place if relative else mine)
            within = (centre - owner * KB + 1).astype(jnp.float32)
            row = jnp.where(at == mark, within, row)
            here = lax.broadcasted_iota(jnp.int32, (META, 128), 0) == rank
            old = out[place, held:, :128].astype(jnp.float32)
            out[place, held:, :128] = jnp.where(here, row, old).astype(out.dtype)


def pack(cfg, start, gates, meta, centers, used, weights, jac):
    count, cap, foot, _ = cfg
    sounds, _, _, cells = jac.shape
    tall = cap * foot * gates + (META if meta else 0)
    scratch = [pltpu.SMEM((count,), jnp.int32)]
    if meta:
        scratch.append(pltpu.VMEM((sounds, 128), jnp.float32))
    args = (centers, used, weights, jac) if meta else (centers, jac)
    return pl.pallas_call(
        functools.partial(pack_kernel, cfg, start, gates, meta),
        out_shape=jax.ShapeDtypeStruct((count, tall, cells), jnp.bfloat16),
        in_specs=[SMEM, SMEM, VMEM, VMEM] if meta else [SMEM, VMEM],
        out_specs=VMEM,
        scratch_shapes=scratch,
        compiler_params=grant(12),
        name="pack",
    )(*args)


def each(count, fn):
    if count <= 32:
        for n in range(count):
            fn(n)
    else:

        def step(n, carry):
            fn(n)
            return carry

        lax.fori_loop(0, count, step, 0)


def part_of(parts, p):
    return parts[p].at[0] if len(parts) > 1 else parts[0].at[p]


def first_kernel(cfg, owners, share, bcap, gates, num, *refs):
    count, cap, foot, _ = cfg
    parts = refs[:num]
    out, table, near, vids, sids, seen, rows, sem = refs[num:]
    span = foot * gates
    slots = share * bcap
    total = jnp.zeros((META, 128), jnp.float32)
    for p in range(count):
        part = part_of(parts, p)[cap * span : cap * span + META, :128].astype(jnp.float32)
        near[p * META : (p + 1) * META, :] = part
        total = total + part
    vids[...] = total.astype(jnp.int32)
    ids = pltpu.make_async_copy(vids, sids, sem)
    ids.start()
    for n in range(KB):
        seen[n] = 0
    rows[...] = jnp.zeros_like(rows)
    out[...] = jnp.zeros_like(out)
    mine = lax.axis_index("rows")
    ids.wait()

    def place(n):
        p = n // cap
        j = n - p * cap
        mark = sids[j, ID_LANE + p]
        table[n] = -1

        @pl.when(mark > 0)
        def _():
            within = mark - 1
            owner = within // share
            row = owner - mine
            row = jnp.where(row < 0, row + owners, row)
            rank = seen[within]
            seen[within] = rank + 1
            slot = (within - owner * share) * bcap + rank
            table[n] = row * slots + slot
            out[row, pl.ds(pl.multiple_of(slot * span, 8), span), :] = part_of(parts, p)[
                pl.ds(j * span, span), :
            ]
            rows[pl.ds(row * META + slot, 1), :] = near[pl.ds(p * META + j, 1), :]

    each(count * cap, place)
    out[:, slots * span :, :128] = (
        rows[...].astype(out.dtype).reshape(owners, META, 128)
    )


def second_kernel(cfg, slots, gates, num, table, *refs):
    count, cap, foot, _ = cfg
    parts = refs[:num]
    (out,) = refs[num:]
    span = foot * gates
    out[...] = jnp.zeros_like(out)

    def place(n):
        p = n // cap
        j = n - p * cap
        to = table[n]

        @pl.when(to >= 0)
        def _():
            row = to // slots
            slot = to - row * slots
            out[row, pl.ds(pl.multiple_of(slot * span, 8), span), :] = part_of(parts, p)[
                pl.ds(j * span, span), :
            ]

    each(count * cap, place)


def bucket_first(cfg, owners, share, bcap, gates, parts):
    count, cap, foot, _ = cfg
    cells = parts[0].shape[2]
    tall = share * bcap * foot * gates + META
    return pl.pallas_call(
        functools.partial(first_kernel, cfg, owners, share, bcap, gates, len(parts)),
        out_shape=(
            jax.ShapeDtypeStruct((owners, tall, cells), jnp.bfloat16),
            jax.ShapeDtypeStruct((count * cap,), jnp.int32),
        ),
        in_specs=[VMEM] * len(parts),
        out_specs=(VMEM, SMEM),
        scratch_shapes=[
            pltpu.VMEM((count * META, 128), jnp.float32),
            pltpu.VMEM((META, 128), jnp.int32),
            pltpu.SMEM((META, 128), jnp.int32),
            pltpu.SMEM((KB,), jnp.int32),
            pltpu.VMEM((owners * META, 128), jnp.float32),
            pltpu.SemaphoreType.DMA(()),
        ],
        compiler_params=grant(12),
        name="bucket",
    )(*parts)


def bucket_second(cfg, owners, slots, gates, table, parts):
    foot = cfg[2]
    cells = parts[0].shape[2]
    return pl.pallas_call(
        functools.partial(second_kernel, cfg, slots, gates, len(parts)),
        out_shape=jax.ShapeDtypeStruct((owners, slots * foot * gates, cells), jnp.bfloat16),
        in_specs=[SMEM] + [VMEM] * len(parts),
        out_specs=VMEM,
        compiler_params=grant(12),
        name="bucket",
    )(table, *parts)


def weight_columns(first, slots, span):
    cols = []
    for ref in first:
        tile = ref[0, slots * span : slots * span + META, :128].astype(jnp.float32)
        cols.append(tile.T)
    return cols


def operands(cols, chunks, block, bcap, foot, i):
    plain, scaled = [], []
    start = 0
    for refs, gates in chunks:
        for q, ref in enumerate(refs):
            for t in range(bcap):
                slot = block * bcap + t
                top = (slot * foot + i) * gates
                rows = ref[0, top : top + gates, :].astype(jnp.float32)
                plain.append(rows)
                scaled.append(rows * cols[q][start : start + gates, slot : slot + 1])
        start += gates
    return (
        jnp.concatenate(plain, axis=0).astype(jnp.bfloat16),
        jnp.concatenate(scaled, axis=0).astype(jnp.bfloat16),
    )


def cross(left, right):
    return lax.dot_general(
        left, right, (((0,), (0,)), ((), ())), preferred_element_type=jnp.float32
    )


def edge_kernel(cfg, gates, num, *refs):
    share, bcap, foot = cfg
    slots = share * bcap
    first, second = refs[:num], refs[num : 2 * num]
    low, high = refs[2 * num :]
    cols = weight_columns(first, slots, foot * gates[0])
    chunks = ((first, gates[0]), (second, gates[1]))
    found = [operands(cols, chunks, 0, bcap, foot, i) for i in range(foot)]
    for d in range(foot):
        low[d] = cross(found[0][1], found[d][0]).astype(low.dtype)
    last = operands(cols, chunks, share - 1, bcap, foot, foot - 1)
    high[0] = cross(last[1], last[0]).astype(high.dtype)


def main_kernel(cfg, gates, num, *refs):
    share, bcap, foot = cfg
    slots = share * bcap
    first, second = refs[:num], refs[num : 2 * num]
    out, edge, hold, sems = refs[2 * num :]
    total = lax.axis_size("blk") * lax.axis_size("rows")
    me = lax.axis_index("blk") * lax.axis_size("rows") + lax.axis_index("rows")
    keep = (me != total - 1).astype(jnp.float32).astype(jnp.bfloat16)
    cols = weight_columns(first, slots, foot * gates[0])
    chunks = ((first, gates[0]), (second, gates[1]))
    found = {}

    def get(j, i):
        if (j, i) not in found:
            found[j, i] = operands(cols, chunks, j, bcap, foot, i)
        return found[j, i]

    def right(j, i, lead):
        rows = get(j, i)[0]
        if j == share - 1 and i == foot - 1 and lead != i:
            rows = rows * keep
        return rows

    copies = []
    for j in range(share):
        for d in range(foot):
            lefts, rights = [], []
            for lead in range(foot - d):
                source = j - lead + 1
                if 0 <= source < share:
                    lefts.append(get(source, lead)[1])
                    rights.append(right(source, lead + d, lead))
            if j == share - 1 or (j == 0 and d == 0):
                spot = edge.at[0 if j == 0 else 1 + d]
            else:
                spot = hold.at[j * foot + d]
            if lefts:
                spot[...] = cross(jnp.concatenate(lefts, 0), jnp.concatenate(rights, 0))
            else:
                spot[...] = jnp.zeros(spot.shape, jnp.float32)
            if not (j == share - 1 or (j == 0 and d == 0)):
                copy = pltpu.make_async_copy(spot, out.at[j, d], sems.at[j * foot + d])
                copy.start()
                copies.append(copy)
    for copy in copies:
        copy.wait()


def join_kernel(share, foot, edge, from_low, from_high, prior, out, hold, sems):
    del prior
    hold[0] = edge[0] + from_low[0].astype(jnp.float32)
    copies = [pltpu.make_async_copy(hold.at[0], out.at[0, 0], sems.at[0])]
    copies[0].start()
    for d in range(foot):
        hold[1 + d] = edge[1 + d] + from_high[d].astype(jnp.float32)
        copy = pltpu.make_async_copy(hold.at[1 + d], out.at[share - 1, d], sems.at[1 + d])
        copy.start()
        copies.append(copy)
    for copy in copies:
        copy.wait()


def over_blk(packed, relative):
    if not relative:
        return [lax.all_to_all(packed, "blk", split_axis=0, concat_axis=0, tiled=True)]
    count = packed.shape[0]
    order = sorted(range(1, count), key=lambda k: abs(2 * k - count))
    parts = {0: packed[0:1]}
    for k in order:
        ring = [(n, (n + k) % count) for n in range(count)]
        parts[k] = lax.ppermute(packed[k : k + 1], "blk", ring)
    return [parts[k] for k in range(count)]


def over_rows(buckets):
    count = buckets.shape[0]
    parts = [buckets[0:1]]
    for k in range(1, count):
        ring = [(n, (n + k) % count) for n in range(count)]
        parts.append(lax.ppermute(buckets[k : k + 1], "rows", ring))
    return parts


def steps(centers, gates_used, jacobian, weights):
    count = lax.axis_size("blk")
    owners = lax.axis_size("rows")
    sounds, foot, gate_len, cells = jacobian.shape
    cap = max(2, 2 * sounds // count)
    bcap = max(2, 2 * sounds // KB)
    share = KB // owners
    slots = share * bcap
    relative = count <= 8
    cfg = (count, cap, foot, relative)
    one = -(-(3 * gate_len // 5) // 8) * 8
    gates = (one, gate_len - one)
    centre_ids = centers[:, 0]

    packed1 = pack(cfg, 0, gates[0], True, centre_ids, gates_used, weights, jacobian)
    arrived1 = over_blk(packed1, relative)
    packed2 = pack(cfg, gates[0], gates[1], False, centre_ids, gates_used, weights, jacobian)
    arrived2 = over_blk(packed2, relative)
    buckets1, table = bucket_first(cfg, owners, share, bcap, gates[0], arrived1)
    first = over_rows(buckets1)
    buckets2 = bucket_second(cfg, owners, slots, gates[1], table, arrived2)
    second = over_rows(buckets2)

    shape = (share, bcap, foot)
    args = (*first, *second)
    low, high = pl.pallas_call(
        functools.partial(edge_kernel, shape, gates, owners),
        out_shape=(
            jax.ShapeDtypeStruct((foot, cells, cells), jnp.bfloat16),
            jax.ShapeDtypeStruct((1, cells, cells), jnp.bfloat16),
        ),
        in_specs=[VMEM] * len(args),
        out_specs=(VMEM, VMEM),
        compiler_params=grant(16),
        name="edge",
    )(*args)
    total = count * owners
    axes = ("blk", "rows")
    from_high = lax.ppermute(low, axes, [(n, n - 1) for n in range(1, total)])
    from_low = lax.ppermute(high, axes, [(n, n + 1) for n in range(total - 1)])
    out_shape = jax.ShapeDtypeStruct((share, foot, cells, cells), jnp.float32)
    inner, edge = pl.pallas_call(
        functools.partial(main_kernel, shape, gates, owners),
        out_shape=(out_shape, jax.ShapeDtypeStruct((1 + foot, cells, cells), jnp.float32)),
        in_specs=[VMEM] * len(args),
        out_specs=(ANY, VMEM),
        scratch_shapes=[
            pltpu.VMEM((share * foot, cells, cells), jnp.float32),
            pltpu.SemaphoreType.DMA((share * foot,)),
        ],
        compiler_params=grant(24),
        name="inner",
    )(*args)
    return pl.pallas_call(
        functools.partial(join_kernel, share, foot),
        out_shape=out_shape,
        in_specs=[VMEM, VMEM, VMEM, ANY],
        out_specs=ANY,
        scratch_shapes=[
            pltpu.VMEM((1 + foot, cells, cells), jnp.float32),
            pltpu.SemaphoreType.DMA((1 + foot,)),
        ],
        input_output_aliases={3: 0},
        compiler_params=grant(8),
        name="join",
    )(edge, from_low, from_high, inner)


def solution(mesh):
    placed = (
        P(("blk", "rows"), None),
        P(("blk", "rows")),
        P(("blk", "rows"), None, None, None),
        P(("blk", "rows"), None),
    )
    return jax.shard_map(
        steps,
        mesh=mesh,
        in_specs=placed,
        out_specs=P(("blk", "rows"), None, None, None),
        check_vma=False,
    )
```
